32 devices in a mesh: row: 8 (over z, y), col: 4 (over x, core).
Axes of the slice: x: 2, y: 2, z: 4, core: 2. Of those that a mesh axis runs over, the one named last changes fastest.
Arguments:
- features: bfloat16 [6144, 4096], P(('row', 'col')), may hold values from -6 to 6
- cotangent: bfloat16 [6144, 8192], P(('row', 'col')), may hold values from -0.078125 to 0.078125
Outputs:
- weight_grad: float32 [4096, 8192], P('row', 'col')
The draws below stay inside these ranges and needn't reach their ends.
All inputs are finite; a program needn't handle non-finite values.
Results may differ from the reference program's by a relative error of at most 0.0003.
Values may be sent and summed in bfloat16 or wider, within the bound.
No kernel may reach another device: no remote copies, remote signals or barrier semaphores. Data moves between devices by JAX's collectives and lax.ppermute only.
A program may use at most 256 MiB of HBM per device.

```python
import jax
import jax.numpy as jnp
from jax import lax

DIN = 4096
DOUT = 8192
TOK_DEV = 192
TOKENS = 6144
N_ROW = 8
N_COL = 4


def strengthened(array, rng, source, target, blocks, factor):
    owner, partner = [(jnp.arange(array.shape[position]) // (array.shape[position] // blocks)).reshape([-1 if axis == position else 1 for axis in range(array.ndim)]) for position in (source, target)]
    chosen = jax.random.permutation(rng, blocks)[partner]
    strong = (owner == chosen) | (owner == (partner + blocks // 2) % blocks)
    return jnp.where(strong, factor * array, array)


def block_levels(own_key, extent, split, low, high):
    def one(position, shards_of):
        heights = jax.random.uniform(jax.random.fold_in(jax.random.fold_in(own_key, 6), position), (shards_of,), jnp.float32, low / len(split), high / len(split))
        return jnp.repeat(jnp.exp(heights), extent[position] // shards_of).reshape((-1,) + (1,) * (len(extent) - position - 1))

    level = one(*split[0])
    for cut in split[1:]:
        level = level * one(*cut)
    return level


def centred(stream_key, shape, width, most, cuts=(), dtype=jnp.bfloat16):
    values = jax.random.normal(stream_key, shape, jnp.float32) * width
    if len(cuts) > 0:
        values = block_levels(stream_key, shape, cuts, -0.22, 0.18) * values
    return jnp.clip(values, min=-most, max=most).astype(dtype)


def heavy_noise(key, shape, deviation, bound, shards, heavy, kind=jnp.bfloat16):
    drawn = deviation * jax.random.normal(key, shape, jnp.float32)
    if shards:
        drawn = drawn * block_levels(key, shape, shards, -0.22, 0.18)
    return jnp.clip(strengthened(drawn, jax.random.fold_in(key, 3), *heavy), -bound, bound).astype(kind)


def setup_inputs(seed: int = 0) -> dict:
    key_of = jax.random.split(jax.random.key(seed), 3)
    features = heavy_noise(key_of[0], (TOKENS, DIN), 1.0, 6.0, ((0, 32),), (0, 1, 32, 2.75))
    cotangent = centred(key_of[1], (TOKENS, DOUT), TOKENS ** -0.5, 0.078125, ((0, 32),))
    return {"features": features, "cotangent": cotangent}


def reference(features, cotangent):
    block_rows = TOK_DEV * N_COL
    feature_blocks = features.reshape(N_ROW, block_rows, DIN)
    cotangent_blocks = cotangent.reshape(N_ROW, block_rows, DOUT)

    def accumulate(running, paired):
        left = paired[0].astype(jnp.float32)
        right = paired[1].astype(jnp.float32)
        return running + jnp.dot(left.T, right, precision=lax.Precision.HIGHEST), None

    initial = jnp.zeros((DIN, DOUT), jnp.float32)
    weight_grad, unused = lax.scan(accumulate, initial, (feature_blocks, cotangent_blocks))
    return weight_grad
```

```python
import functools

import jax
import jax.numpy as jnp
from jax import lax
from jax.experimental import pallas as pl
from jax.experimental.pallas import tpu as pltpu
from jax.sharding import PartitionSpec as P

AXES = ("row", "col")
SCALE_ROWS = 8
LIFT = 2.0**7.5
STRIP = 128


def factors(mesh):
    devices = mesh.devices
    rows, cols = devices.shape
    gather, cores = 1, 1
    spots = [getattr(d, "coords", None) for d in devices[:, 0]]
    if None not in spots and rows > 1:
        moved = [i for i in range(3) if spots[0][i] != spots[1][i]]
        if len(moved) == 1:
            gather = len({s[moved[0]] for s in spots})
    sides = [getattr(d, "coords", None) for d in devices[0, :]]
    if cols % 2 == 0 and (sides[0] is None or tuple(sides[0]) == tuple(sides[1])):
        cores = 2
    if rows % gather:
        gather = 1
    return rows // gather, gather, cols // cores, cores


def slots_of(line):
    slots = []
    for r in range(1, line):
        up = {z: line - r + z for z in range(line) if z <= r - 1}
        down = {z: r + z - line for z in range(line) if z >= line - r}
        if 2 * r <= line:
            slots.append((r, "both", up, down))
        else:
            slots.append((r, "up", up, {}))
            slots.append((r, "down", {}, down))
    return slots


def decoded(ref, rows, height):
    code = ref[rows, :].astype(jnp.float32)
    scale = ref[height : height + SCALE_ROWS, :].astype(jnp.float32)[0:1] * (1.0 / LIFT)
    size = jnp.exp(jnp.log(jnp.abs(code)) * (1.0 / 16.0)) * scale
    return jnp.where(code < 0, -size, jnp.where(code > 0, size, 0.0))


def strip_product(left_refs, right, rows):
    left = jnp.concatenate([ref[:, rows] for ref in left_refs], axis=0)
    return lax.dot_general(
        left, right, (((0,), (0,)), ((), ())), preferred_element_type=jnp.float32
    )


def right_tokens(refs, cores):
    tokens = refs[0].shape[0] // cores
    return jnp.concatenate(
        [ref[k * tokens : (k + 1) * tokens, :] for k in range(cores) for ref in refs], axis=0
    )


def send_kernel(n_left, n_right, n_recv, cores, *refs):
    left, refs = refs[:n_left], refs[n_left:]
    right, refs = refs[:n_right], refs[n_right:]
    recv, refs = refs[:n_recv], refs[n_recv:]
    out, total, peak = refs[-3:]
    height, width = total.shape
    strip = min(STRIP, height)
    peak[...] = jnp.zeros_like(peak)

    @pl.loop(0, height // strip)
    def _(i):
        rows = pl.ds(pl.multiple_of(i * strip, strip), strip)
        value = strip_product(left, right_tokens(right, cores), rows)
        for ref in recv:
            value = value + decoded(ref, rows, height)
        total[rows, :] = value
        peak[...] = jnp.maximum(
            peak[...], jnp.max(jnp.abs(value).reshape(-1, 8, width), axis=0)
        )

    scale = jnp.max(peak[...], axis=0, keepdims=True).astype(jnp.bfloat16)
    wide = scale.astype(jnp.float32)
    lift = jnp.where(wide > 1e-30, LIFT / jnp.maximum(wide, 1e-30), 0.0)
    out[height : height + SCALE_ROWS, :] = jnp.broadcast_to(wide, (SCALE_ROWS, width)).astype(
        out.dtype
    )

    @pl.loop(0, height // strip)
    def _(i):
        rows = pl.ds(pl.multiple_of(i * strip, strip), strip)
        value = total[rows, :]
        power = jnp.abs(value) * lift
        for _ in range(4):
            power = power * power
        out[rows, :] = jnp.where(value < 0, -power, power).astype(out.dtype)


def last_kernel(n_left, n_right, n_recv, cores, *refs):
    left, refs = refs[:n_left], refs[n_left:]
    right, refs = refs[:n_right], refs[n_right:]
    recv, refs = refs[:n_recv], refs[n_recv:]
    out = refs[-1]
    height = out.shape[0]
    strip = min(STRIP, height)

    @pl.loop(0, height // strip)
    def _(i):
        rows = pl.ds(pl.multiple_of(i * strip, strip), strip)
        value = strip_product(left, right_tokens(right, cores), rows)
        for ref in recv:
            value = value + decoded(ref, rows, height)
        out[rows, :] = value


def whole_spec(array):
    return pl.BlockSpec(array.shape, lambda i: (0, 0))


def cost(height, width, depth, moved):
    return pl.CostEstimate(
        flops=2 * height * width * depth, bytes_accessed=moved, transcendentals=2 * height * width
    )


ANY = pl.BlockSpec(memory_space=pl.ANY)


def send_step(left, right, recv, after, height, cores):
    width = right[0].shape[1]
    depth = sum(a.shape[0] for a in left)
    operands = [*left, *right, *recv]
    return pl.pallas_call(
        functools.partial(send_kernel, len(left), len(right), len(recv), cores),
        grid=(1,),
        in_specs=[whole_spec(a) for a in operands] + [ANY] * len(after),
        out_specs=pl.BlockSpec((height + SCALE_ROWS, width), lambda i: (0, 0)),
        out_shape=jax.ShapeDtypeStruct((height + SCALE_ROWS, width), jnp.bfloat16),
        scratch_shapes=[
            pltpu.VMEM((height, width), jnp.float32),
            pltpu.VMEM((8, width), jnp.float32),
        ],
        cost_estimate=cost(height, width, depth, sum(a.size * 2 for a in operands)),
        name="send_step",
    )(*operands, *after)


def last_step(left, right, recv, after, buffer, height, full, column, cores):
    width = right[0].shape[1]
    depth = sum(a.shape[0] for a in left)
    operands = [*left, *right, *recv]
    extra = [*after] if buffer is None else [*after, buffer]
    return pl.pallas_call(
        functools.partial(last_kernel, len(left), len(right), len(recv), cores),
        grid=(1,),
        in_specs=[whole_spec(a) for a in operands] + [ANY] * len(extra),
        out_specs=pl.BlockSpec((height, width), lambda i: (0, column)),
        out_shape=jax.ShapeDtypeStruct((height, full), jnp.float32),
        input_output_aliases={} if buffer is None else {len(operands) + len(extra) - 1: 0},
        cost_estimate=cost(height, width, depth, sum(a.size * 2 for a in operands)),
        name="last_step",
    )(*operands, *extra)


def local(shape, features, cotangent):
    line, gather, sides, cores = shape
    tokens = features.shape[0]
    height = features.shape[1] // (line * gather)
    width = cotangent.shape[1] // (sides * cores)
    pieces = 4 if width % 512 == 0 else 1
    chunk = width // pieces
    row, col = lax.axis_index("row"), lax.axis_index("col")
    z, y = row // gather, row % gather
    x, core = col // cores, col % cores

    def moves(target, planes=None):
        pairs = []
        for a in range(line) if planes is None else planes:
            for b in range(gather):
                for c in range(sides):
                    for k in range(cores):
                        a2, b2, c2, k2 = target(a, b, c, k)
                        source = (a * gather + b) * sides * cores + c * cores + k
                        pairs.append((source, (a2 * gather + b2) * sides * cores + c2 * cores + k2))
        return pairs

    def partner(array):
        return lax.ppermute(array, AXES, moves(lambda a, b, c, k: (a, b, c, 1 - k)))

    offsets = [(dx, dy) for dy in range(gather) for dx in range(sides)]

    def in_plane(payloads, planes=None):
        got = []
        for (dx, dy), payload in zip(offsets, payloads):
            if dx == 0 and dy == 0:
                got.append(payload)
            else:
                pairs = moves(
                    lambda a, b, c, k: (a, (b + dy) % gather, (c + dx) % sides, k), planes
                )
                got.append(lax.ppermute(payload, AXES, pairs))
        return got

    def left_block(table, planes):
        block = jnp.array([table.get(a, 0) for a in range(line)], jnp.int32)[z]
        cut = {
            dy: lax.dynamic_slice_in_dim(
                features, (block * gather + (y + dy) % gather) * height, height, axis=1
            )
            for dy in range(gather)
        }
        mine = jnp.concatenate(in_plane([cut[dy] for _, dy in offsets], planes), axis=0)
        return [mine, partner(mine)] if cores == 2 else [mine]

    def right_chunk(index):
        def cut(dx, k):
            start = (((x + dx) % sides) * cores + k) * width + index * chunk
            return lax.dynamic_slice_in_dim(cotangent, start, chunk, axis=1)

        mine = [cut(dx, core) for dx in range(sides)]
        if cores == 2:
            other = partner(jnp.concatenate([cut(dx, 1 - core) for dx in range(sides)], axis=0))
            mine = [
                jnp.concatenate([m, other[dx * tokens : (dx + 1) * tokens]], axis=0)
                for dx, m in enumerate(mine)
            ]
        return in_plane([mine[dx] for dx, _ in offsets])

    slots = slots_of(line)
    lefts, rights = [], []
    for index, (_, _, up, down) in enumerate(slots):
        lefts.append(left_block({**up, **down}, sorted({**up, **down})))
        if index == 0:
            rights.append(right_chunk(0))
    own = left_block({a: a for a in range(line)}, None)
    while len(rights) < pieces:
        rights.append(right_chunk(len(rights)))

    def shift(array, planes, step):
        return lax.ppermute(array, AXES, moves(lambda a, b, c, k: (a + step, b, c, k), planes))

    state = [None] * pieces
    after, buffer = [], None

    def round_of(r, c):
        nonlocal after
        came = state[c]
        next_up, next_down = None, None
        for index, (rr, way, up, down) in enumerate(slots):
            if rr != r:
                continue
            recv = []
            if came is not None:
                both, from_below, from_above = came
                recv = [m for m in (both, from_below if up else None, from_above if down else None) if m is not None]
            message = send_step(lefts[index], rights[c], recv, after, height, cores)
            after = [message]
            if way == "both" and not {a + 1 for a in up} & {a - 1 for a in down}:
                pairs = moves(lambda a, b, c, k: (a + 1, b, c, k), sorted(up)) + moves(
                    lambda a, b, c, k: (a - 1, b, c, k), sorted(down)
                )
                state[c] = (lax.ppermute(message, AXES, pairs), None, None)
                return
            if up:
                next_up = shift(message, sorted(up), 1)
            if down:
                next_down = shift(message, sorted(down), -1)
        state[c] = (None, next_up, next_down)

    def finish(c):
        nonlocal after, buffer
        recv = [m for m in (state[c] or ()) if m is not None]
        buffer = last_step(own, rights[c], recv, after, buffer, height, width, c, cores)
        after = []

    waiting = []
    for first in range(0, pieces, 2):
        pair = [c for c in (first, first + 1) if c < pieces]
        for r in range(1, line):
            for c in pair:
                round_of(r, c)
            if r == 1:
                for c in waiting:
                    finish(c)
                waiting = []
        waiting = pair
    for c in waiting:
        finish(c)
    return buffer


def solution(mesh):
    placed = (P(AXES, None), P(AXES, None))
    return jax.shard_map(
        functools.partial(local, factors(mesh)),
        mesh=mesh,
        in_specs=placed,
        out_specs=P("row", "col"),
        check_vma=False,
    )
```
